32 devices in a mesh: dp: 1 (over z), tp: 4 (over y), cp: 8 (over x, core).
Axes of the slice: x: 4, y: 4, z: 1, core: 2. Of those that a mesh axis runs over, the one named last changes fastest.
The devices are a block of a 4x4x8 slice.
Arguments:
- x: bfloat16 [2048, 6144], P(('dp', 'cp'))
- k_cache: bfloat16 [65536, 8, 128], P(('dp', 'cp'), 'tp')
- v_cache: bfloat16 [65536, 8, 128], P(('dp', 'cp'), 'tp')
- rope_table: float32 [2048, 64], P(('dp', 'cp'))
- norm_gain: bfloat16 [6144], replicated
- w_qkv: bfloat16 [6144, 8192], P(None, 'tp')
- b_qkv: bfloat16 [8192], P('tp')
- w_out: bfloat16 [6144, 6144], P('tp')
Outputs:
- output 1: bfloat16 [2048, 6144], P(('dp', 'cp'))
- output 2: bfloat16 [2048, 8, 128], P(('dp', 'cp'), 'tp')
- output 3: bfloat16 [2048, 8, 128], P(('dp', 'cp'), 'tp')
All inputs are finite; a program needn't handle non-finite values.
Results may differ from the reference program's by a relative error of at most 0.00313401.
Values are sent between devices in bfloat16 or wider.
A program may use at most 768 MiB of HBM per device.

```python
import math
import jax
import jax.numpy as jnp
from jax import lax

D = 6144
HEADS = 48
KV_HEADS = 8
HEAD = 128
NEW_TOKENS = 2048
PREFIX = 65536
EPS = 1.5625e-07
MASK_VALUE = -1e30
GROUP = HEADS // KV_HEADS
QKV_WIDTH = (HEADS + 2 * KV_HEADS) * HEAD
PAIR_COUNT = HEAD // 4
QUERY_BLOCK = math.gcd(NEW_TOKENS, 128)
KEY_BLOCK = math.gcd(PREFIX + NEW_TOKENS, 512)


def setup_inputs(seed: int = 0, part: int = 0) -> dict:
    part_keys = jax.random.split(jax.random.fold_in(jax.random.key(seed), part), 4)
    shared_keys = jax.random.split(jax.random.key(seed + 1), 4)
    x = jax.random.normal(part_keys[0], (NEW_TOKENS, D), jnp.float32)
    k_cache = 1.6 * jax.random.normal(part_keys[1], (PREFIX, KV_HEADS, HEAD), jnp.float32)
    v_cache = 1.6 * jax.random.normal(part_keys[2], (PREFIX, KV_HEADS, HEAD), jnp.float32)
    log_ratio = jax.random.uniform(part_keys[3], (), jnp.float32, math.log(100.0), math.log(10000.0))
    rope_base = 10000.0 * jnp.exp(log_ratio)
    inv_freq = rope_base ** (-jnp.arange(PAIR_COUNT, dtype=jnp.float32) / PAIR_COUNT)
    positions = (PREFIX + jnp.arange(NEW_TOKENS)).astype(jnp.float32)
    angles = positions[:, None] * inv_freq[None, :]
    rope_table = jnp.concatenate([jnp.cos(angles), jnp.sin(angles)], axis=1)
    norm_gain = 1.0 + 0.3 * jax.random.normal(shared_keys[0], (D,), jnp.float32)
    w_qkv = jax.random.normal(shared_keys[1], (D, QKV_WIDTH), jnp.float32) * (1.5 / math.sqrt(D))
    b_qkv = 0.5 * jax.random.normal(shared_keys[2], (QKV_WIDTH,), jnp.float32)
    w_out = jax.random.normal(shared_keys[3], (HEADS * HEAD, D), jnp.float32) / math.sqrt(HEADS * HEAD)
    return dict(x=x.astype(jnp.bfloat16), k_cache=k_cache.astype(jnp.bfloat16), v_cache=v_cache.astype(jnp.bfloat16), rope_table=rope_table.astype(jnp.float32), norm_gain=norm_gain.astype(jnp.bfloat16), w_qkv=w_qkv.astype(jnp.bfloat16), b_qkv=b_qkv.astype(jnp.bfloat16), w_out=w_out.astype(jnp.bfloat16))


def apply_rotary(vals, cos_t, sin_t):
    pair_count = cos_t.shape[-1]
    lead_shape = vals.shape[:-1]
    paired = vals[..., :2 * pair_count].reshape(lead_shape + (pair_count, 2))
    even_part = paired[..., 0]
    odd_part = paired[..., 1]
    turned = jnp.stack([even_part * cos_t - odd_part * sin_t, odd_part * cos_t + even_part * sin_t], axis=-1)
    return jnp.concatenate([turned.reshape(lead_shape + (2 * pair_count,)), vals[..., 2 * pair_count:]], axis=-1)


def reference(x, k_cache, v_cache, rope_table, norm_gain, w_qkv, b_qkv, w_out):
    x_f32 = x.astype(jnp.float32)
    inv_rms = lax.rsqrt(jnp.mean(x_f32 * x_f32, axis=-1, keepdims=True) + EPS)
    hidden = (x_f32 * inv_rms * norm_gain.astype(jnp.float32)).astype(jnp.bfloat16)
    qkv_all = jnp.dot(hidden, w_qkv, preferred_element_type=jnp.float32) + b_qkv.astype(jnp.float32)
    qkv_all = qkv_all.reshape(NEW_TOKENS, KV_HEADS, GROUP + 2, HEAD)
    cos_t = rope_table[:, :PAIR_COUNT]
    sin_t = rope_table[:, PAIR_COUNT:]
    queries = apply_rotary(qkv_all[:, :, :GROUP], cos_t[:, None, None], sin_t[:, None, None]).astype(jnp.bfloat16)
    new_k = apply_rotary(qkv_all[:, :, GROUP], cos_t[:, None], sin_t[:, None]).astype(jnp.bfloat16)
    new_v = qkv_all[:, :, GROUP + 1].astype(jnp.bfloat16)
    key_count = PREFIX + NEW_TOKENS
    key_blocks = key_count // KEY_BLOCK
    keys_all = jnp.concatenate([k_cache, new_k], axis=0).reshape(key_blocks, KEY_BLOCK, KV_HEADS, HEAD)
    vals_all = jnp.concatenate([v_cache, new_v], axis=0).reshape(key_blocks, KEY_BLOCK, KV_HEADS, HEAD)
    key_pos = jnp.arange(key_count).reshape(key_blocks, KEY_BLOCK)
    q_blocks = queries.reshape(NEW_TOKENS // QUERY_BLOCK, QUERY_BLOCK, KV_HEADS, GROUP, HEAD)
    q_pos = (PREFIX + jnp.arange(NEW_TOKENS)).reshape(NEW_TOKENS // QUERY_BLOCK, QUERY_BLOCK)
    scale = HEAD ** -0.5

    def query_block(block):
        q_vals, q_at = block
        q_f32 = q_vals.astype(jnp.float32)

        def key_step(carry, kv_block):
            run_max, run_sum, weighted = carry
            k_vals, v_vals, k_at = kv_block
            scores = jnp.einsum('qngd,knd->qngk', q_f32, k_vals.astype(jnp.float32)) * scale
            visible = (k_at[None, :] <= q_at[:, None])[:, None, None, :]
            scores = jnp.where(visible, scores, MASK_VALUE)
            new_max = jnp.maximum(run_max, scores.max(axis=-1))
            rescale = jnp.exp(run_max - new_max)
            probs = jnp.exp(scores - new_max[..., None])
            run_sum = run_sum * rescale + probs.sum(axis=-1)
            weighted = weighted * rescale[..., None] + jnp.einsum('qngk,knd->qngd', probs.astype(jnp.bfloat16).astype(jnp.float32), v_vals.astype(jnp.float32))
            return (new_max, run_sum, weighted), None

        start_carry = (jnp.full((QUERY_BLOCK, KV_HEADS, GROUP), MASK_VALUE, jnp.float32), jnp.zeros((QUERY_BLOCK, KV_HEADS, GROUP), jnp.float32), jnp.zeros((QUERY_BLOCK, KV_HEADS, GROUP, HEAD), jnp.float32))
        (run_max, run_sum, weighted), _ = lax.scan(key_step, start_carry, (keys_all, vals_all, key_pos))
        return weighted / run_sum[..., None]

    attn = lax.map(query_block, (q_blocks, q_pos))
    attn = attn.reshape(NEW_TOKENS, HEADS * HEAD).astype(jnp.bfloat16)
    y = (x_f32 + jnp.dot(attn, w_out, preferred_element_type=jnp.float32)).astype(jnp.bfloat16)
    return y, new_k, new_v
```

```python
import functools
import math

import jax
import jax.numpy as jnp
from jax import lax
from jax.experimental import pallas as pl
from jax.experimental.pallas import tpu as pltpu
from jax.sharding import PartitionSpec as P

EPS = 1.5625e-07
MASK_VALUE = -1e30
LIMIT = 1e30
F32, BF16 = jnp.float32, jnp.bfloat16
STATS = 8


def project_kernel(heads, dim, x_ref, gain_ref, w_ref, b_ref, cos_ref, sin_ref, nat_ref, tr_ref, h_ref):
    step = pl.program_id(0)
    rows = x_ref.shape[0]
    width = w_ref.shape[1]

    @pl.when(step == 0)
    def _():
        def norm(i, _):
            at = pl.ds(pl.multiple_of(i * 16, 16), 16)
            xf = x_ref[at, :].astype(F32)
            inv = lax.rsqrt(jnp.mean(xf * xf, axis=-1, keepdims=True) + EPS)
            h_ref[at, :] = (xf * inv * gain_ref[...].astype(F32)).astype(BF16)
            return 0
        lax.fori_loop(0, rows // 16, norm, 0)

    a = jnp.dot(h_ref[...], w_ref[...], preferred_element_type=F32) + b_ref[...].astype(F32)
    lane = lax.broadcasted_iota(jnp.int32, (rows, dim), 1)
    for part in range(width // dim):
        v = a[:, part * dim:(part + 1) * dim]
        swapped = jnp.where(lane % 2 == 0, pltpu.roll(v, dim - 1, 1), pltpu.roll(v, 1, 1))
        turned = v * cos_ref[...] + swapped * sin_ref[...]
        head = lax.rem(step * (width // dim) + part, heads)
        keep = jnp.where(head == heads - 1, 0, dim // 2)
        out = jnp.where(lane < keep, turned, v)
        nat_ref[:, part * dim:(part + 1) * dim] = out.astype(BF16)
        tr_ref[part * dim:(part + 1) * dim, :] = out.T.astype(BF16)


def project(x, rope_table, norm_gain, w_qkv, b_qkv, heads, dim):
    rows, d_model = x.shape
    cols = w_qkv.shape[1]
    pairs = rope_table.shape[1] // 2
    cos_t, sin_t = rope_table[:, :pairs], rope_table[:, pairs:]
    pad = dim - 2 * pairs
    cos_w = jnp.concatenate([jnp.repeat(cos_t, 2, axis=1), jnp.ones((rows, pad), F32)], axis=1)
    sin_w = jnp.concatenate([jnp.stack([-sin_t, sin_t], axis=-1).reshape(rows, 2 * pairs), jnp.zeros((rows, pad), F32)], axis=1)
    width = 2 * dim
    return pl.pallas_call(
        functools.partial(project_kernel, heads, dim),
        grid=(cols // width,),
        in_specs=[
            pl.BlockSpec((rows, d_model), lambda i: (0, 0)),
            pl.BlockSpec((1, d_model), lambda i: (0, 0)),
            pl.BlockSpec((d_model, width), lambda i: (0, i)),
            pl.BlockSpec((1, width), lambda i: (0, i)),
            pl.BlockSpec((rows, dim), lambda i: (0, 0)),
            pl.BlockSpec((rows, dim), lambda i: (0, 0)),
        ],
        out_specs=[pl.BlockSpec((rows, width), lambda i: (0, i)), pl.BlockSpec((width, rows), lambda i: (i, 0))],
        out_shape=[jax.ShapeDtypeStruct((rows, cols), BF16), jax.ShapeDtypeStruct((cols, rows), BF16)],
        scratch_shapes=[pltpu.VMEM((rows, d_model), BF16)],
        compiler_params=pltpu.CompilerParams(vmem_limit_bytes=40 * 2**20, dimension_semantics=("arbitrary",)),
        cost_estimate=pl.CostEstimate(flops=2 * rows * d_model * cols, bytes_accessed=2 * d_model * cols, transcendentals=0),
        name="project",
    )(x, norm_gain[None, :], w_qkv, b_qkv[None, :], cos_w, sin_w)


def attend_kernel(c, blocks, bk, sub, shift_ref, *refs):
    q_refs = refs[:blocks]
    k_ref, vt_ref, kn_ref, vnt_ref = refs[blocks:blocks + 4]
    out_refs = refs[blocks + 4:2 * blocks + 4]
    acc_ref = refs[2 * blocks + 4]
    heads, dim, toks = q_refs[0].shape[1:]
    cols = heads * toks
    nk, nn = k_ref.shape[1], kn_ref.shape[1]
    q = jnp.concatenate([r[0, h] for r in q_refs for h in range(heads)], axis=1)
    bq = q.shape[1]

    def scores(k):
        return jnp.dot(k, q, preferred_element_type=F32)

    def fold(p):
        return jnp.sum(p.reshape(p.shape[0] // 8, 8, bq), axis=0)

    def new_scores():
        s = scores(kn_ref[0])
        ahead = lax.broadcasted_iota(jnp.int32, (nn, toks), 0) - lax.broadcasted_iota(jnp.int32, (nn, toks), 1)
        parts = []
        for b in range(blocks):
            vis = ahead <= shift_ref[b]
            for h in range(heads):
                at = b * cols + h * toks
                parts.append(jnp.where(vis, s[:, at:at + toks], MASK_VALUE))
        return jnp.concatenate(parts, axis=1)

    top = jnp.max(scores(k_ref[0, :256, :]), axis=0, keepdims=True) * c
    p = jnp.exp2(new_scores() * c - top)
    row_sum = fold(p)
    acc_ref[...] = jnp.dot(vnt_ref[0], p.astype(BF16), preferred_element_type=F32)

    def body(i, row_sum):
        base = pl.multiple_of(i * bk, bk)
        acc = None
        for j in range(bk // sub):
            at = pl.ds(base + j * sub, sub)
            p = jnp.exp2(scores(k_ref[0, at, :]) * c - top)
            row_sum = row_sum + fold(p)
            d = jnp.dot(vt_ref[0, :, at], p.astype(BF16), preferred_element_type=F32)
            acc = d if acc is None else acc + d
        acc_ref[...] += acc
        return row_sum

    row_sum = jnp.sum(lax.fori_loop(0, nk // bk, body, row_sum), axis=0, keepdims=True)

    def emit(top, row_sum):
        for b in range(blocks):
            at = slice(b * cols, (b + 1) * cols)
            out_refs[b][0, :dim] = acc_ref[:, at]
            out_refs[b][0, dim:dim + STATS] = jnp.concatenate([top[:, at], row_sum[:, at], jnp.zeros((STATS - 2, cols), F32)], axis=0)

    emit(top, row_sum)
    worst = jnp.maximum(jnp.max(jnp.abs(acc_ref[...])), jnp.max(row_sum))

    @pl.when(jnp.logical_not(worst < LIMIT))
    def _():
        acc_ref[...] = jnp.zeros_like(acc_ref)

        def update(s, vt, carry):
            m, l = carry
            new = jnp.maximum(m, jnp.max(s, axis=0, keepdims=True) * c)
            r = jnp.exp2(m - new)
            p = jnp.exp2(s * c - new)
            acc_ref[...] = acc_ref[...] * r + jnp.dot(vt, p.astype(BF16), preferred_element_type=F32)
            return new, l * r + jnp.sum(p, axis=0, keepdims=True)

        def slow(i, carry):
            at = pl.ds(pl.multiple_of(i * 256, 256), 256)
            return update(scores(k_ref[0, at, :]), vt_ref[0, :, at], carry)

        carry = (jnp.full((1, bq), MASK_VALUE, F32), jnp.zeros((1, bq), F32))
        carry = lax.fori_loop(0, nk // 256, slow, carry)
        emit(*update(new_scores(), vnt_ref[0], carry))


def attend(qs, shifts, k, vt, kn, vnt, bk=4096, sub=2048):
    blocks = len(qs)
    groups, heads, dim, toks = qs[0].shape
    nk, nn = k.shape[1], kn.shape[1]
    cols = heads * toks
    c = math.log2(math.e) * dim ** -0.5
    grid_spec = pltpu.PrefetchScalarGridSpec(
        num_scalar_prefetch=1,
        grid=(groups,),
        in_specs=[pl.BlockSpec((1, heads, dim, toks), lambda i, s: (i, 0, 0, 0))] * blocks + [
            pl.BlockSpec((1, nk, dim), lambda i, s: (i, 0, 0)),
            pl.BlockSpec((1, dim, nk), lambda i, s: (i, 0, 0)),
            pl.BlockSpec((1, nn, dim), lambda i, s: (i, 0, 0)),
            pl.BlockSpec((1, dim, nn), lambda i, s: (i, 0, 0)),
        ],
        out_specs=[pl.BlockSpec((1, dim + STATS, cols), lambda i, s: (i, 0, 0))] * blocks,
        scratch_shapes=[pltpu.VMEM((dim, blocks * cols), F32)],
    )
    return pl.pallas_call(
        functools.partial(attend_kernel, c, blocks, bk, sub),
        grid_spec=grid_spec,
        out_shape=[jax.ShapeDtypeStruct((groups, dim + STATS, cols), F32)] * blocks,
        compiler_params=pltpu.CompilerParams(vmem_limit_bytes=62 * 2**20, dimension_semantics=("arbitrary",)),
        cost_estimate=pl.CostEstimate(flops=4 * groups * blocks * cols * (nk + nn) * dim, bytes_accessed=4 * groups * nk * dim, transcendentals=groups * blocks * cols * nk),
        name="attend",
    )(shifts, *qs, k, vt, kn, vnt)


def merge(parts, dim):
    tops = [p[:, dim:dim + 1] for p in parts]
    top = functools.reduce(jnp.maximum, tops)
    scales = [jnp.exp2(t - top) for t in tops]
    total = sum(p[:, dim + 1:dim + 2] * s for p, s in zip(parts, scales))
    acc = sum(p[:, :dim] * s for p, s in zip(parts, scales))
    return (acc / total).astype(BF16)


def ring(size, k):
    return [(i, (i + k) % size) for i in range(size)]


def make_step(cp_size, tp_size):
    def local_step(x, k_cache, v_cache, rope_table, norm_gain, w_qkv, b_qkv, w_out):
        groups, dim = k_cache.shape[1], k_cache.shape[2]
        rows, d_model = x.shape
        group_cols = w_qkv.shape[1] // groups
        heads = group_cols // dim
        q_heads = heads - 2
        me = lax.axis_index('cp')
        tp_me = lax.axis_index('tp')
        odd = lax.rem(me, 2)
        nat, tr = project(x, rope_table, norm_gain, w_qkv, b_qkv, heads, dim)
        nat = nat.reshape(rows, groups, heads, dim)
        tr = tr.reshape(groups, heads, dim, rows)
        k_new, v_new = nat[:, :, q_heads], nat[:, :, q_heads + 1]
        kn = k_new.transpose(1, 0, 2)
        vnt = tr[:, q_heads + 1]
        k_loc = k_cache.transpose(1, 0, 2)
        vt_loc = v_cache.transpose(1, 2, 0)

        w_rows = w_out.shape[0]
        half = w_rows // 2
        quarter = d_model // tp_size
        mine, other = [], []
        swap = [(i, i ^ 1) for i in range(cp_size)]
        for k in range(tp_size):
            to = lax.rem(tp_me + k, tp_size)
            if k == 0:
                piece = lax.dynamic_slice(w_out, (0, to * quarter), (w_rows, quarter))
                mine.append(piece)
                continue
            piece = lax.dynamic_slice(w_out, (odd * half, to * quarter), (half, quarter))
            piece = lax.ppermute(piece, 'tp', ring(tp_size, k))
            mine.append(piece)
            other.append(lax.ppermute(piece, 'cp', swap))

        toks = rows // 2
        x_f32 = x.astype(F32)
        ys = []
        orders = [[(0, 1), (cp_size - 1, 2), (cp_size - 2, 3), (cp_size - 3, 4)], [(4, cp_size - 3), (3, cp_size - 2), (2, cp_size - 1), (1, 0)]]
        q_parts = []
        for chunk in range(2):
            q_own = tr[:, :q_heads, :, chunk * toks:(chunk + 1) * toks]
            q_parts.append([q_own if k == 0 else lax.ppermute(q_own, 'cp', ring(cp_size, -k)) for k in range(cp_size)])
        for chunk in range(2):
            got = []
            for pair in orders[chunk]:
                shifts = jnp.stack([(lax.rem(me + k, cp_size) - me) * rows + chunk * toks for k in pair]).astype(jnp.int32)
                outs = attend([q_parts[chunk][k] for k in pair], shifts, k_loc, vt_loc, kn, vnt)
                for k, out in zip(pair, outs):
                    got.append(out if k == 0 else lax.ppermute(out, 'cp', ring(cp_size, k)))
            o = merge(got, dim).reshape(groups, dim, q_heads, toks).transpose(0, 2, 1, 3).reshape(w_rows, toks)
            acc = x_f32[chunk * toks:(chunk + 1) * toks]
            acc = lax.dynamic_slice(acc, (0, tp_me * quarter), (toks, quarter))
            prod = functools.partial(lax.dot_general, dimension_numbers=(((0,), (0,)), ((), ())), preferred_element_type=F32)
            total = prod(o, mine[0])
            for k in range(1, tp_size):
                o_k = lax.ppermute(o, 'tp', ring(tp_size, k))
                total += prod(lax.dynamic_slice(o_k, (odd * half, 0), (half, toks)), mine[k])
                total += prod(lax.dynamic_slice(o_k, ((1 - odd) * half, 0), (half, toks)), other[k - 1])
            y = (acc + total).astype(BF16)
            pieces = [y] + [lax.ppermute(y, 'tp', ring(tp_size, k)) for k in range(1, tp_size)]
            full = jnp.zeros((toks, d_model), BF16)
            for k, piece in enumerate(pieces):
                full = lax.dynamic_update_slice(full, piece, (0, lax.rem(tp_me - k + tp_size, tp_size) * quarter))
            ys.append(full)
        return jnp.concatenate(ys, axis=0), k_new, v_new
    return local_step


def solution(mesh):
    row_spec = P(('dp', 'cp'), None)
    cache_spec = P(('dp', 'cp'), 'tp', None)
    step = make_step(mesh.shape['cp'], mesh.shape['tp'])
    return jax.shard_map(step, mesh=mesh, in_specs=(row_spec, cache_spec, cache_spec, row_spec, P(None), P(None, 'tp'), P('tp'), P('tp', None)), out_specs=(row_spec, cache_spec, cache_spec), check_vma=False)
```

```python
import functools
import math

import jax
import jax.numpy as jnp
from jax import lax
from jax.experimental import pallas as pl
from jax.experimental.pallas import tpu as pltpu
from jax.sharding import PartitionSpec as P


EPS = 1.5625e-07
MASK_VALUE = -1e30
LIMIT = 1e30
F32, BF16 = jnp.float32, jnp.bfloat16
STATS = 8
RELAYED = 0


def project_kernel(heads, dim, x_ref, gain_ref, w_ref, b_ref, cos_ref, sin_ref, nat_ref, tr_ref, h_ref):
    step = pl.program_id(0)
    rows = x_ref.shape[0]
    width = w_ref.shape[1]

    @pl.when(step == 0)
    def _():
        def norm(i, _):
            at = pl.ds(pl.multiple_of(i * 16, 16), 16)
            xf = x_ref[at, :].astype(F32)
            inv = lax.rsqrt(jnp.mean(xf * xf, axis=-1, keepdims=True) + EPS)
            h_ref[at, :] = (xf * inv * gain_ref[...].astype(F32)).astype(BF16)
            return 0

        lax.fori_loop(0, rows // 16, norm, 0)

    a = jnp.dot(h_ref[...], w_ref[...], preferred_element_type=F32) + b_ref[...].astype(F32)
    lane = lax.broadcasted_iota(jnp.int32, (rows, dim), 1)
    for part in range(width // dim):
        v = a[:, part * dim:(part + 1) * dim]
        swapped = jnp.where(lane % 2 == 0, pltpu.roll(v, dim - 1, 1), pltpu.roll(v, 1, 1))
        turned = v * cos_ref[...] + swapped * sin_ref[...]
        head = lax.rem(step * (width // dim) + part, heads)
        keep = jnp.where(head == heads - 1, 0, dim // 2)
        out = jnp.where(lane < keep, turned, v)
        nat_ref[:, part * dim:(part + 1) * dim] = out.astype(BF16)
        tr_ref[part * dim:(part + 1) * dim, :] = out.T.astype(BF16)


def project(x, rope_table, norm_gain, w_qkv, b_qkv, heads, dim):
    rows, d_model = x.shape
    cols = w_qkv.shape[1]
    pairs = rope_table.shape[1] // 2
    lane = jnp.arange(dim)[None, :]
    pair = jnp.arange(pairs)[:, None]
    cos_pick = (lane // 2 == pair).astype(F32)
    sin_pick = cos_pick * jnp.where(lane % 2 == 0, -1.0, 1.0)
    zero = jnp.zeros_like(cos_pick)
    pick = jnp.concatenate([jnp.concatenate([cos_pick, zero], axis=1), jnp.concatenate([zero, sin_pick], axis=1)], axis=0)
    wide = jnp.dot(rope_table, pick, precision=lax.Precision.HIGHEST, preferred_element_type=F32)
    cos_w, sin_w = wide[:, :dim], wide[:, dim:]
    width = 2 * dim
    return pl.pallas_call(
        functools.partial(project_kernel, heads, dim),
        grid=(cols // width,),
        in_specs=[
            pl.BlockSpec((rows, d_model), lambda i: (0, 0)),
            pl.BlockSpec((1, d_model), lambda i: (0, 0)),
            pl.BlockSpec((d_model, width), lambda i: (0, i)),
            pl.BlockSpec((1, width), lambda i: (0, i)),
            pl.BlockSpec((rows, dim), lambda i: (0, 0)),
            pl.BlockSpec((rows, dim), lambda i: (0, 0)),
        ],
        out_specs=[pl.BlockSpec((rows, width), lambda i: (0, i)), pl.BlockSpec((width, rows), lambda i: (i, 0))],
        out_shape=[jax.ShapeDtypeStruct((rows, cols), BF16), jax.ShapeDtypeStruct((cols, rows), BF16)],
        scratch_shapes=[pltpu.VMEM((rows, d_model), BF16)],
        compiler_params=pltpu.CompilerParams(vmem_limit_bytes=40 * 2**20, dimension_semantics=("arbitrary",)),
        cost_estimate=pl.CostEstimate(flops=2 * rows * d_model * cols, bytes_accessed=2 * d_model * cols, transcendentals=0),
        name="project",
    )(x, norm_gain[None, :], w_qkv, b_qkv[None, :], cos_w, sin_w)


def attend_kernel(c, blocks, bk, sub, shift_ref, *refs):
    q_refs = refs[:blocks]
    k_ref, vt_ref, kn_ref, vnt_ref = refs[blocks:blocks + 4]
    out_refs = refs[blocks + 4:2 * blocks + 4]
    acc_ref = refs[2 * blocks + 4]
    heads, dim, toks = q_refs[0].shape[1:]
    cols = heads * toks
    nk, nn = k_ref.shape[1], kn_ref.shape[1]
    q = jnp.concatenate([r[0, h] for r in q_refs for h in range(heads)], axis=1)
    bq = q.shape[1]

    def scores(k):
        return jnp.dot(k, q, preferred_element_type=F32)

    def fold(p):
        return jnp.sum(p.reshape(p.shape[0] // 8, 8, bq), axis=0)

    top = jnp.max(scores(k_ref[0, :256, :]), axis=0, keepdims=True)
    high = top.astype(BF16).astype(F32)
    mid = (top - high).astype(BF16).astype(F32)
    low = top - high - mid
    row = lax.broadcasted_iota(jnp.int32, (dim, bq), 0)
    bias = jnp.where(row == 0, high, jnp.where(row == 1, mid, jnp.where(row == 2, low, 0.0)))
    q_ext = jnp.concatenate([q, (-bias).astype(BF16)], axis=0)

    def shifted(k):
        ones = jnp.ones((k.shape[0], dim), BF16)
        return jnp.dot(jnp.concatenate([k, ones], axis=1), q_ext, preferred_element_type=F32)

    def mask_new(s):
        ahead = lax.broadcasted_iota(jnp.int32, (nn, toks), 0) - lax.broadcasted_iota(jnp.int32, (nn, toks), 1)
        parts = []
        for b in range(blocks):
            vis = ahead <= shift_ref[b]
            for h in range(heads):
                at = b * cols + h * toks
                parts.append(jnp.where(vis, s[:, at:at + toks], MASK_VALUE))
        return jnp.concatenate(parts, axis=1)

    p = jnp.exp2(mask_new(shifted(kn_ref[0])) * c)
    row_sum = fold(p)
    acc_ref[...] = jnp.dot(vnt_ref[0], p.astype(BF16), preferred_element_type=F32)

    def body(i, row_sum):
        base = pl.multiple_of(i * bk, bk)
        acc = None
        for j in range(bk // sub):
            at = pl.ds(base + j * sub, sub)
            p = jnp.exp2(shifted(k_ref[0, at, :]) * c)
            row_sum = row_sum + fold(p)
            d = jnp.dot(vt_ref[0, :, at], p.astype(BF16), preferred_element_type=F32)
            acc = d if acc is None else acc + d
        acc_ref[...] += acc
        return row_sum

    row_sum = jnp.sum(lax.fori_loop(0, nk // bk, body, row_sum), axis=0, keepdims=True)

    def emit(top, row_sum):
        for b in range(blocks):
            at = slice(b * cols, (b + 1) * cols)
            out_refs[b][0, :dim] = acc_ref[:, at]
            out_refs[b][0, dim:dim + STATS] = jnp.concatenate([top[:, at], row_sum[:, at], jnp.zeros((STATS - 2, cols), F32)], axis=0)

    emit(top * c, row_sum)
    worst = jnp.maximum(jnp.max(jnp.abs(acc_ref[...])), jnp.max(row_sum))

    @pl.when(jnp.logical_not(worst < LIMIT))
    def _():
        acc_ref[...] = jnp.zeros_like(acc_ref)

        def update(s, vt, carry):
            m, l = carry
            new = jnp.maximum(m, jnp.max(s, axis=0, keepdims=True) * c)
            r = jnp.exp2(m - new)
            p = jnp.exp2(s * c - new)
            acc_ref[...] = acc_ref[...] * r + jnp.dot(vt, p.astype(BF16), preferred_element_type=F32)
            return new, l * r + jnp.sum(p, axis=0, keepdims=True)

        def slow(i, carry):
            at = pl.ds(pl.multiple_of(i * 256, 256), 256)
            return update(scores(k_ref[0, at, :]), vt_ref[0, :, at], carry)

        carry = (jnp.full((1, bq), MASK_VALUE, F32), jnp.zeros((1, bq), F32))
        carry = lax.fori_loop(0, nk // 256, slow, carry)
        emit(*update(mask_new(scores(kn_ref[0])), vnt_ref[0], carry))


def attend(qs, shifts, k, vt, kn, vnt, toks, at=0, bk=2048, sub=1024):
    blocks = len(qs)
    groups, heads, dim, _ = qs[0].shape
    nk, nn = k.shape[1], kn.shape[1]
    cols = heads * toks
    c = math.log2(math.e) * dim ** -0.5
    grid_spec = pltpu.PrefetchScalarGridSpec(
        num_scalar_prefetch=1,
        grid=(groups,),
        in_specs=[pl.BlockSpec((1, heads, dim, toks), lambda i, s: (i, 0, 0, at))] * blocks + [
            pl.BlockSpec((1, nk, dim), lambda i, s: (i, 0, 0)),
            pl.BlockSpec((1, dim, nk), lambda i, s: (i, 0, 0)),
            pl.BlockSpec((1, nn, dim), lambda i, s: (i, 0, 0)),
            pl.BlockSpec((1, dim, nn), lambda i, s: (i, 0, 0)),
        ],
        out_specs=[pl.BlockSpec((1, dim + STATS, cols), lambda i, s: (i, 0, 0))] * blocks,
        scratch_shapes=[pltpu.VMEM((dim, blocks * cols), F32)],
    )
    return pl.pallas_call(
        functools.partial(attend_kernel, c, blocks, bk, sub),
        grid_spec=grid_spec,
        out_shape=[jax.ShapeDtypeStruct((groups, dim + STATS, cols), F32)] * blocks,
        compiler_params=pltpu.CompilerParams(vmem_limit_bytes=62 * 2**20, dimension_semantics=("arbitrary",)),
        cost_estimate=pl.CostEstimate(flops=4 * groups * blocks * cols * (nk + nn) * dim, bytes_accessed=4 * groups * nk * dim, transcendentals=groups * blocks * cols * nk),
        name="attend",
    )(shifts, *qs, k, vt, kn, vnt)


def tail_kernel(remote, groups, heads, dim, *refs):
    parts = refs[:remote]
    x_ref, w_own = refs[remote:remote + 2]
    w_mine, w_other = refs[remote + 2:remote + 5], refs[remote + 5:remote + 8]
    y_ref, pbuf, wbuf, xbuf, o_own, o_left, o_right, o_far, acc, load, wload, send, recv = refs[remote + 8:]
    rows, quarter = acc.shape
    toks = rows // 2
    wide = heads * dim
    tp, cp = lax.axis_index('tp'), lax.axis_index('cp')
    odd = lax.rem(cp, 2)
    left, right = lax.rem(tp + 3, 4), lax.rem(tp + 1, 4)

    barrier = pltpu.get_barrier_semaphore()
    for to in (left, right):
        pl.semaphore_signal(barrier, inc=1, device_id={'tp': to}, device_id_type=pl.DeviceIdType.MESH)

    loads = []
    for g in range(groups):
        here = [pltpu.make_async_copy(p.at[g], pbuf.at[g, i], load.at[g, i]) for i, p in enumerate(parts)]
        for d in here:
            d.start()
        loads.append(here)
    wloads = [pltpu.make_async_copy(x_ref.at[:, pl.ds(pl.multiple_of(tp * quarter, quarter), quarter)], xbuf, wload.at[0])]
    for g in range(groups):
        wloads.append(pltpu.make_async_copy(w_own.at[pl.ds(g * wide, wide), pl.ds(pl.multiple_of(tp * quarter, quarter), quarter)], wbuf.at[0, g], wload.at[1 + g]))
    for k in range(3):
        wloads.append(pltpu.make_async_copy(w_mine[k], wbuf.at[k + 1, odd], wload.at[3 + 2 * k]))
        wloads.append(pltpu.make_async_copy(w_other[k], wbuf.at[k + 1, 1 - odd], wload.at[4 + 2 * k]))
    for d in wloads:
        d.start()

    def remote_copy(src, dst, i, to):
        return pltpu.make_async_remote_copy(src_ref=src, dst_ref=dst, send_sem=send.at[i], recv_sem=recv.at[i], device_id={'tp': to}, device_id_type=pl.DeviceIdType.MESH)

    def merge(g):
        for d in loads[g]:
            d.wait()

        for h in range(heads):
            at = slice(h * rows, (h + 1) * rows)
            tops = [pbuf[g, i, dim:dim + 1, at] for i in range(remote)]
            sums = [pbuf[g, i, dim + 1:dim + 2, at] for i in range(remote)]
            top = functools.reduce(jnp.maximum, tops)
            scales = [jnp.exp2(t - top) for t in tops]
            total = sum(l * s for l, s in zip(sums, scales))
            val = sum(pbuf[g, i, :dim, at] * scales[i] for i in range(remote))
            o_own[g, :, h * dim:(h + 1) * dim] = (val / total).T.astype(BF16)

    def product(o, g, k, row=0, n=None, first=False):
        n = rows if n is None else n

        @pl.loop(0, quarter // 512)
        def _(j):
            at = pl.ds(pl.multiple_of(j * 512, 512), 512)
            d = jnp.dot(o[g, row:row + n, :], wbuf[k, g, :, at], preferred_element_type=F32)
            acc[row:row + n, at] = d if first else acc[row:row + n, at] + d

    merge(0)
    pl.semaphore_wait(barrier, 2)
    c0r = remote_copy(o_own.at[0], o_left.at[0], 0, right)
    c0l = remote_copy(o_own.at[0], o_right.at[0], 1, left)
    c0r.start()
    c0l.start()
    merge(1)
    c1l = remote_copy(o_own.at[1], o_right.at[1], 2, left)
    c1r = remote_copy(o_own.at[1], o_left.at[1], 3, right)
    c1l.start()
    c1r.start()
    for d in wloads:
        d.wait()
    product(o_own, 0, 0, first=True)
    product(o_own, 1, 0)
    c0r.wait_recv()
    f0 = remote_copy(o_left.at[0], o_far.at[0], 4, right)
    f0.start()
    c0l.wait_recv()
    product(o_left, 0, 1)
    product(o_right, 0, 3)
    c1l.wait_recv()
    f1 = remote_copy(o_right.at[1], o_far.at[1], 5, left)
    f1.start()
    c1r.wait_recv()
    product(o_right, 1, 3)
    product(o_left, 1, 1)
    f0.wait_recv()
    f1.wait_recv()

    def cols(t):
        return pl.ds(pl.multiple_of(t * quarter, quarter), quarter)

    def block(r, t):
        return y_ref.at[pl.ds(r * toks, toks), cols(t)]

    copies = [c0r, c0l, c1l, c1r, f0, f1]
    ycopies = []
    for r in range(2):
        product(o_far, 0, 2, r * toks, toks)
        product(o_far, 1, 2, r * toks, toks)
        at = slice(r * toks, (r + 1) * toks)
        y_ref[at, cols(tp)] = (xbuf[at].astype(F32) + acc[at]).astype(BF16)
        for i, to in enumerate((right, left) if r == 0 else (left, right)):
            d = remote_copy(block(r, tp), block(r, tp), 6 + 2 * r + i, to)
            d.start()
            ycopies.append(d)
    ar, al, bl, br = ycopies
    ar.wait_recv()
    fa = remote_copy(block(0, left), block(0, left), 10, right)
    fa.start()
    bl.wait_recv()
    fb = remote_copy(block(1, right), block(1, right), 11, left)
    fb.start()
    al.wait_recv()
    br.wait_recv()
    fa.wait_recv()
    fb.wait_recv()
    for d in copies + ycopies + [fa, fb]:
        d.wait_send()


def tail(parts, x, w_own, w_mine, w_other, heads, dim):
    groups = parts[0].shape[0]
    rows, d_model = x.shape
    quarter = w_mine[0].shape[1]
    wide = heads * dim
    remote = len(parts)
    any_spec = pl.BlockSpec(memory_space=pl.ANY)
    return pl.pallas_call(
        functools.partial(tail_kernel, remote, groups, heads, dim),
        out_shape=jax.ShapeDtypeStruct((rows, d_model), BF16),
        in_specs=[any_spec] * (remote + 8),
        out_specs=pl.BlockSpec(memory_space=pltpu.VMEM),
        scratch_shapes=[
            pltpu.VMEM((groups, remote) + parts[0].shape[1:], F32),
            pltpu.VMEM((4, groups, wide, quarter), BF16),
            pltpu.VMEM((rows, quarter), BF16),
            pltpu.VMEM((groups, rows, wide), BF16),
            pltpu.VMEM((groups, rows, wide), BF16),
            pltpu.VMEM((groups, rows, wide), BF16),
            pltpu.VMEM((groups, rows, wide), BF16),
            pltpu.VMEM((rows, quarter), F32),
            pltpu.SemaphoreType.DMA((groups, remote)),
            pltpu.SemaphoreType.DMA((9,)),
            pltpu.SemaphoreType.DMA((12,)),
            pltpu.SemaphoreType.DMA((12,)),
        ],
        compiler_params=pltpu.CompilerParams(vmem_limit_bytes=60 * 2**20, collective_id=0, has_side_effects=True),
        cost_estimate=pl.CostEstimate(flops=2 * rows * d_model * groups * wide, bytes_accessed=2 * d_model * quarter, transcendentals=0),
        name="tail",
    )(*parts, x, w_own, *w_mine, *w_other)


def ring(size, k):
    return [(i, (i + k) % size) for i in range(size)]


def make_step(cp_size, tp_size):
    def local_step(x, k_cache, v_cache, rope_table, norm_gain, w_qkv, b_qkv, w_out):
        groups, dim = k_cache.shape[1], k_cache.shape[2]
        rows, d_model = x.shape
        group_cols = w_qkv.shape[1] // groups
        heads = group_cols // dim
        q_heads = heads - 2
        me = lax.axis_index('cp')
        tp_me = lax.axis_index('tp')
        odd = lax.rem(me, 2)
        nat, tr = project(x, rope_table, norm_gain, w_qkv, b_qkv, heads, dim)
        nat = nat.reshape(rows, groups, heads, dim)
        tr = tr.reshape(groups, heads, dim, rows)
        k_new, v_new = nat[:, :, q_heads], nat[:, :, q_heads + 1]
        kn = k_new.transpose(1, 0, 2)
        vnt = tr[:, q_heads + 1]
        k_loc = k_cache.transpose(1, 0, 2)
        vt_loc = v_cache.transpose(1, 2, 0)

        q_own = tr[:, :q_heads]
        chips = cp_size // 2
        order = ((2, 1), (2, 0), (3, 0), (1, 0), (3, 1), (1, 1), (0, 1))

        def hop(val, j, flip):
            return lax.ppermute(val, 'cp', [(i, (i // 2 + j) % chips * 2 + (i % 2 ^ flip)) for i in range(cp_size)])

        def run(q, j, flip):
            owner = lax.rem(me // 2 + j, chips) * 2 + lax.rem(me + flip, 2)
            shifts = jnp.stack([(owner - me) * rows]).astype(jnp.int32)
            return attend([q], shifts, k_loc, vt_loc, kn, vnt, rows)[0]

        q10 = hop(q_own, -1, 0)
        q30 = hop(q_own, 1, 0)
        own = run(q_own, 0, 0)
        w_late, q10_late, own = lax.optimization_barrier((w_out, q10, own))
        q21 = hop(q10_late, -1, 1)
        q20 = hop(q21, 0, 1)
        queries = [q21, q20, q30, q10, hop(q30, 0, 1), hop(q10, 0, 1), hop(q_own, 0, 1)]

        w_rows = w_out.shape[0]
        half = w_rows // 2
        quarter = d_model // tp_size
        swap = [(i, i ^ 1) for i in range(cp_size)]
        mine, other = [], []
        for k in range(1, tp_size):
            to = lax.rem(tp_me + k, tp_size)
            piece = lax.dynamic_slice(w_late, (odd * half, to * quarter), (half, quarter))
            piece = lax.ppermute(piece, 'tp', ring(tp_size, k))
            mine.append(piece)

        parts, moving, last = [], None, own
        for n, q in enumerate(queries):
            if n == RELAYED + 2:
                q, last, moving = lax.optimization_barrier((q, last, moving))
                parts.append(hop(moving, -1, order[RELAYED][1]))
            elif n == len(order) - 1:
                q, last, mine = lax.optimization_barrier((q, last, mine))
                for piece in mine:
                    other.append(lax.ppermute(piece, 'cp', swap))
            else:
                q, last = lax.optimization_barrier((q, last))
            out = last = run(q, *order[n])
            if n == RELAYED:
                moving = hop(out, -1, 0)
            else:
                parts.append(hop(out, *order[n]))
        y = tail(parts + [own], x, w_out, mine, other, q_heads, dim)
        return y, k_new, v_new

    return local_step


def solution(mesh):
    row_spec = P(('dp', 'cp'), None)
    cache_spec = P(('dp', 'cp'), 'tp', None)
    inner = make_step(mesh.shape['cp'], mesh.shape['tp'])

    return jax.shard_map(inner, mesh=mesh, in_specs=(row_spec, cache_spec, cache_spec, row_spec, P(None), P(None, 'tp'), P('tp'), P('tp', None)), out_specs=(row_spec, cache_spec, cache_spec), check_vma=False)
```

```python
import functools
import math

import jax
import jax.numpy as jnp
from jax import lax
from jax.experimental import pallas as pl
from jax.experimental.pallas import tpu as pltpu
from jax.sharding import PartitionSpec as P


EPS = 1.5625e-07
MASK_VALUE = -1e30
SUM_LIMIT = 1e12
ACC_LIMIT = 1e36
F32, BF16 = jnp.float32, jnp.bfloat16
STATS = 8
RELAYED = 0


def project_kernel(heads, dim, x_ref, gain_ref, w_ref, b_ref, cos_ref, sin_ref, nat_ref, tr_ref, h_ref):
    step = pl.program_id(0)
    rows = x_ref.shape[0]
    width = w_ref.shape[1]

    @pl.when(step == 0)
    def _():
        def norm(i, _):
            at = pl.ds(pl.multiple_of(i * 16, 16), 16)
            xf = x_ref[at, :].astype(F32)
            inv = lax.rsqrt(jnp.mean(xf * xf, axis=-1, keepdims=True) + EPS)
            h_ref[at, :] = (xf * inv * gain_ref[...].astype(F32)).astype(BF16)
            return 0

        lax.fori_loop(0, rows // 16, norm, 0)

    a = jnp.dot(h_ref[...], w_ref[...], preferred_element_type=F32) + b_ref[...].astype(F32)
    lane = lax.broadcasted_iota(jnp.int32, (rows, dim), 1)
    for part in range(width // dim):
        v = a[:, part * dim:(part + 1) * dim]
        swapped = jnp.where(lane % 2 == 0, pltpu.roll(v, dim - 1, 1), pltpu.roll(v, 1, 1))
        turned = v * cos_ref[...] + swapped * sin_ref[...]
        head = lax.rem(step * (width // dim) + part, heads)
        keep = jnp.where(head == heads - 1, 0, dim // 2)
        out = jnp.where(lane < keep, turned, v)
        nat_ref[:, part * dim:(part + 1) * dim] = out.astype(BF16)
        tr_ref[part * dim:(part + 1) * dim, :] = out.T.astype(BF16)


def project(x, rope_table, norm_gain, w_qkv, b_qkv, heads, dim):
    rows, d_model = x.shape
    cols = w_qkv.shape[1]
    pairs = rope_table.shape[1] // 2
    lane = jnp.arange(dim)[None, :]
    pair = jnp.arange(pairs)[:, None]
    cos_pick = (lane // 2 == pair).astype(F32)
    sin_pick = cos_pick * jnp.where(lane % 2 == 0, -1.0, 1.0)
    zero = jnp.zeros_like(cos_pick)
    pick = jnp.concatenate([jnp.concatenate([cos_pick, zero], axis=1), jnp.concatenate([zero, sin_pick], axis=1)], axis=0)
    wide = jnp.dot(rope_table, pick, precision=lax.Precision.HIGHEST, preferred_element_type=F32)
    cos_w, sin_w = wide[:, :dim], wide[:, dim:]
    width = 2 * dim
    return pl.pallas_call(
        functools.partial(project_kernel, heads, dim),
        grid=(cols // width,),
        in_specs=[
            pl.BlockSpec((rows, d_model), lambda i: (0, 0)),
            pl.BlockSpec((1, d_model), lambda i: (0, 0)),
            pl.BlockSpec((d_model, width), lambda i: (0, i)),
            pl.BlockSpec((1, width), lambda i: (0, i)),
            pl.BlockSpec((rows, dim), lambda i: (0, 0)),
            pl.BlockSpec((rows, dim), lambda i: (0, 0)),
        ],
        out_specs=[pl.BlockSpec((rows, width), lambda i: (0, i)), pl.BlockSpec((width, rows), lambda i: (i, 0))],
        out_shape=[jax.ShapeDtypeStruct((rows, cols), BF16), jax.ShapeDtypeStruct((cols, rows), BF16)],
        scratch_shapes=[pltpu.VMEM((rows, d_model), BF16)],
        compiler_params=pltpu.CompilerParams(vmem_limit_bytes=40 * 2**20, dimension_semantics=("arbitrary",)),
        cost_estimate=pl.CostEstimate(flops=2 * rows * d_model * cols, bytes_accessed=2 * d_model * cols, transcendentals=0),
        name="project",
    )(x, norm_gain[None, :], w_qkv, b_qkv[None, :], cos_w, sin_w)


def attend_kernel(c, blocks, bk, sub, shift_ref, *refs):
    q_refs = refs[:blocks]
    k_ref, vt_ref, kn_ref, vnt_ref = refs[blocks:blocks + 4]
    out_refs = refs[blocks + 4:2 * blocks + 4]
    acc_ref = refs[2 * blocks + 4]
    heads, dim, toks = q_refs[0].shape[1:]
    cols = heads * toks
    nk, nn = k_ref.shape[1], kn_ref.shape[1]
    q = jnp.concatenate([r[0, h] for r in q_refs for h in range(heads)], axis=1)
    bq = q.shape[1]

    def scores(k):
        return jnp.dot(k, q, preferred_element_type=F32)

    def fold(p):
        return jnp.sum(p.reshape(p.shape[0] // 8, 8, bq), axis=0)

    top = jnp.max(scores(k_ref[0, :256, :]), axis=0, keepdims=True)
    high = top.astype(BF16).astype(F32)
    mid = (top - high).astype(BF16).astype(F32)
    low = top - high - mid
    row = lax.broadcasted_iota(jnp.int32, (dim, bq), 0)
    bias = jnp.where(row == 0, high, jnp.where(row == 1, mid, jnp.where(row == 2, low, 0.0)))
    q_ext = jnp.concatenate([q, (-bias).astype(BF16)], axis=0)

    def shifted(k):
        ones = jnp.ones((k.shape[0], dim), BF16)
        return jnp.dot(jnp.concatenate([k, ones], axis=1), q_ext, preferred_element_type=F32)

    def mask_new(s):
        ahead = lax.broadcasted_iota(jnp.int32, (nn, toks), 0) - lax.broadcasted_iota(jnp.int32, (nn, toks), 1)
        parts = []
        for b in range(blocks):
            vis = ahead <= shift_ref[b]
            for h in range(heads):
                at = b * cols + h * toks
                parts.append(jnp.where(vis, s[:, at:at + toks], MASK_VALUE))
        return jnp.concatenate(parts, axis=1)

    p = jnp.exp2(mask_new(shifted(kn_ref[0])) * c)
    row_sum = fold(p)
    acc_ref[...] = jnp.dot(vnt_ref[0], p.astype(BF16), preferred_element_type=F32)

    def body(i, row_sum):
        base = pl.multiple_of(i * bk, bk)
        acc = None
        for j in range(bk // sub):
            at = pl.ds(base + j * sub, sub)
            p = jnp.exp2(shifted(k_ref[0, at, :]) * c)
            row_sum = row_sum + fold(p)
            d = jnp.dot(vt_ref[0, :, at], p.astype(BF16), preferred_element_type=F32)
            acc = d if acc is None else acc + d
        acc_ref[...] += acc
        return row_sum

    row_sum = jnp.sum(lax.fori_loop(0, nk // bk, body, row_sum), axis=0, keepdims=True)

    def emit(top, row_sum):
        for b in range(blocks):
            at = slice(b * cols, (b + 1) * cols)
            out_refs[b][0, :dim] = acc_ref[:, at]
            out_refs[b][0, dim:dim + STATS] = jnp.concatenate([top[:, at], row_sum[:, at], jnp.zeros((STATS - 2, cols), F32)], axis=0)

    emit(top * c, row_sum)
    fits = jnp.logical_and(jnp.max(row_sum) < SUM_LIMIT, jnp.max(jnp.abs(acc_ref[...])) < ACC_LIMIT)

    @pl.when(jnp.logical_not(fits))
    def _():
        def head(h, _):
            at = pl.ds(pl.multiple_of(h * toks, toks), toks)
            for b in range(blocks):
                qh = q_refs[b][0, h]

                def update(s, vt, carry):
                    m, l, acc = carry
                    new = jnp.maximum(m, jnp.max(s, axis=0, keepdims=True) * c)
                    r = jnp.exp2(m - new)
                    p = jnp.exp2(s * c - new)
                    acc = acc * r + jnp.dot(vt, p.astype(BF16), preferred_element_type=F32)
                    return new, l * r + jnp.sum(p, axis=0, keepdims=True), acc

                def slow(i, carry):
                    keys = pl.ds(pl.multiple_of(i * 256, 256), 256)
                    return update(jnp.dot(k_ref[0, keys, :], qh, preferred_element_type=F32), vt_ref[0, :, keys], carry)

                carry = (jnp.full((1, toks), MASK_VALUE, F32), jnp.zeros((1, toks), F32), jnp.zeros((dim, toks), F32))
                carry = lax.fori_loop(0, nk // 256, slow, carry)
                ahead = lax.broadcasted_iota(jnp.int32, (nn, toks), 0) - lax.broadcasted_iota(jnp.int32, (nn, toks), 1)
                s = jnp.where(ahead <= shift_ref[b], jnp.dot(kn_ref[0], qh, preferred_element_type=F32), MASK_VALUE)
                m, l, acc = update(s, vnt_ref[0], carry)
                out_refs[b][0, :dim, at] = acc
                out_refs[b][0, dim:dim + STATS, at] = jnp.concatenate([m, l, jnp.zeros((STATS - 2, toks), F32)], axis=0)
            return 0

        lax.fori_loop(0, heads, head, 0)


def attend(qs, shifts, k, vt, kn, vnt, toks, at=0, bk=2048, sub=1024):
    blocks = len(qs)
    groups, heads, dim, _ = qs[0].shape
    nk, nn = k.shape[1], kn.shape[1]
    cols = heads * toks
    c = math.log2(math.e) * dim ** -0.5
    grid_spec = pltpu.PrefetchScalarGridSpec(
        num_scalar_prefetch=1,
        grid=(groups,),
        in_specs=[pl.BlockSpec((1, heads, dim, toks), lambda i, s: (i, 0, 0, at))] * blocks + [
            pl.BlockSpec((1, nk, dim), lambda i, s: (i, 0, 0)),
            pl.BlockSpec((1, dim, nk), lambda i, s: (i, 0, 0)),
            pl.BlockSpec((1, nn, dim), lambda i, s: (i, 0, 0)),
            pl.BlockSpec((1, dim, nn), lambda i, s: (i, 0, 0)),
        ],
        out_specs=[pl.BlockSpec((1, dim + STATS, cols), lambda i, s: (i, 0, 0))] * blocks,
        scratch_shapes=[pltpu.VMEM((dim, blocks * cols), F32)],
    )
    return pl.pallas_call(
        functools.partial(attend_kernel, c, blocks, bk, sub),
        grid_spec=grid_spec,
        out_shape=[jax.ShapeDtypeStruct((groups, dim + STATS, cols), F32)] * blocks,
        compiler_params=pltpu.CompilerParams(vmem_limit_bytes=62 * 2**20, dimension_semantics=("arbitrary",)),
        cost_estimate=pl.CostEstimate(flops=4 * groups * blocks * cols * (nk + nn) * dim, bytes_accessed=4 * groups * nk * dim, transcendentals=groups * blocks * cols * nk),
        name="attend",
    )(shifts, *qs, k, vt, kn, vnt)


def tail_kernel(remote, groups, heads, dim, *refs):
    parts = refs[:remote]
    x_ref, w_own = refs[remote:remote + 2]
    w_mine, w_other = refs[remote + 2:remote + 5], refs[remote + 5:remote + 8]
    y_ref, pbuf, wbuf, xbuf, o_own, o_left, o_right, o_far, acc, load, wload, send, recv = refs[remote + 8:]
    rows, quarter = acc.shape
    toks = rows // 2
    wide = heads * dim
    tp, cp = lax.axis_index('tp'), lax.axis_index('cp')
    odd = lax.rem(cp, 2)
    left, right = lax.rem(tp + 3, 4), lax.rem(tp + 1, 4)

    barrier = pltpu.get_barrier_semaphore()
    for to in (left, right):
        pl.semaphore_signal(barrier, inc=1, device_id={'tp': to}, device_id_type=pl.DeviceIdType.MESH)

    loads = []
    for g in range(groups):
        here = [pltpu.make_async_copy(p.at[g], pbuf.at[g, i], load.at[g, i]) for i, p in enumerate(parts)]
        for d in here:
            d.start()
        loads.append(here)
    wloads = [pltpu.make_async_copy(x_ref.at[:, pl.ds(pl.multiple_of(tp * quarter, quarter), quarter)], xbuf, wload.at[0])]
    for g in range(groups):
        wloads.append(pltpu.make_async_copy(w_own.at[pl.ds(g * wide, wide), pl.ds(pl.multiple_of(tp * quarter, quarter), quarter)], wbuf.at[0, g], wload.at[1 + g]))
    for k in range(3):
        wloads.append(pltpu.make_async_copy(w_mine[k], wbuf.at[k + 1, odd], wload.at[3 + 2 * k]))
        wloads.append(pltpu.make_async_copy(w_other[k], wbuf.at[k + 1, 1 - odd], wload.at[4 + 2 * k]))
    for d in wloads:
        d.start()

    def remote_copy(src, dst, i, to):
        return pltpu.make_async_remote_copy(src_ref=src, dst_ref=dst, send_sem=send.at[i], recv_sem=recv.at[i], device_id={'tp': to}, device_id_type=pl.DeviceIdType.MESH)

    def merge(g):
        for d in loads[g]:
            d.wait()

        for h in range(heads):
            at = slice(h * rows, (h + 1) * rows)
            tops = [pbuf[g, i, dim:dim + 1, at] for i in range(remote)]
            sums = [pbuf[g, i, dim + 1:dim + 2, at] for i in range(remote)]
            top = functools.reduce(jnp.maximum, tops)
            scales = [jnp.exp2(t - top) for t in tops]
            total = sum(l * s for l, s in zip(sums, scales))
            val = sum(pbuf[g, i, :dim, at] * scales[i] for i in range(remote))
            o_own[g, :, h * dim:(h + 1) * dim] = (val / total).T.astype(BF16)

    def product(o, g, k, row=0, n=None, first=False):
        n = rows if n is None else n

        @pl.loop(0, quarter // 512)
        def _(j):
            at = pl.ds(pl.multiple_of(j * 512, 512), 512)
            d = jnp.dot(o[g, row:row + n, :], wbuf[k, g, :, at], preferred_element_type=F32)
            acc[row:row + n, at] = d if first else acc[row:row + n, at] + d

    merge(0)
    pl.semaphore_wait(barrier, 2)
    c0r = remote_copy(o_own.at[0], o_left.at[0], 0, right)
    c0l = remote_copy(o_own.at[0], o_right.at[0], 1, left)
    c0r.start()
    c0l.start()
    merge(1)
    c1l = remote_copy(o_own.at[1], o_right.at[1], 2, left)
    c1r = remote_copy(o_own.at[1], o_left.at[1], 3, right)
    c1l.start()
    c1r.start()
    for d in wloads:
        d.wait()
    product(o_own, 0, 0, first=True)
    product(o_own, 1, 0)
    c0r.wait_recv()
    f0 = remote_copy(o_left.at[0], o_far.at[0], 4, right)
    f0.start()
    c0l.wait_recv()
    product(o_left, 0, 1)
    product(o_right, 0, 3)
    c1l.wait_recv()
    f1 = remote_copy(o_right.at[1], o_far.at[1], 5, left)
    f1.start()
    c1r.wait_recv()
    product(o_right, 1, 3)
    product(o_left, 1, 1)
    f0.wait_recv()
    f1.wait_recv()

    def cols(t):
        return pl.ds(pl.multiple_of(t * quarter, quarter), quarter)

    def block(r, t):
        return y_ref.at[pl.ds(r * toks, toks), cols(t)]

    copies = [c0r, c0l, c1l, c1r, f0, f1]
    ycopies = []
    for r in range(2):
        product(o_far, 0, 2, r * toks, toks)
        product(o_far, 1, 2, r * toks, toks)
        at = slice(r * toks, (r + 1) * toks)
        y_ref[at, cols(tp)] = (xbuf[at].astype(F32) + acc[at]).astype(BF16)
        for i, to in enumerate((right, left) if r == 0 else (left, right)):
            d = remote_copy(block(r, tp), block(r, tp), 6 + 2 * r + i, to)
            d.start()
            ycopies.append(d)
    ar, al, bl, br = ycopies
    ar.wait_recv()
    fa = remote_copy(block(0, left), block(0, left), 10, right)
    fa.start()
    bl.wait_recv()
    fb = remote_copy(block(1, right), block(1, right), 11, left)
    fb.start()
    al.wait_recv()
    br.wait_recv()
    fa.wait_recv()
    fb.wait_recv()
    for d in copies + ycopies + [fa, fb]:
        d.wait_send()


def tail(parts, x, w_own, w_mine, w_other, heads, dim):
    groups = parts[0].shape[0]
    rows, d_model = x.shape
    quarter = w_mine[0].shape[1]
    wide = heads * dim
    remote = len(parts)
    any_spec = pl.BlockSpec(memory_space=pl.ANY)
    return pl.pallas_call(
        functools.partial(tail_kernel, remote, groups, heads, dim),
        out_shape=jax.ShapeDtypeStruct((rows, d_model), BF16),
        in_specs=[any_spec] * (remote + 8),
        out_specs=pl.BlockSpec(memory_space=pltpu.VMEM),
        scratch_shapes=[
            pltpu.VMEM((groups, remote) + parts[0].shape[1:], F32),
            pltpu.VMEM((4, groups, wide, quarter), BF16),
            pltpu.VMEM((rows, quarter), BF16),
            pltpu.VMEM((groups, rows, wide), BF16),
            pltpu.VMEM((groups, rows, wide), BF16),
            pltpu.VMEM((groups, rows, wide), BF16),
            pltpu.VMEM((groups, rows, wide), BF16),
            pltpu.VMEM((rows, quarter), F32),
            pltpu.SemaphoreType.DMA((groups, remote)),
            pltpu.SemaphoreType.DMA((9,)),
            pltpu.SemaphoreType.DMA((12,)),
            pltpu.SemaphoreType.DMA((12,)),
        ],
        compiler_params=pltpu.CompilerParams(vmem_limit_bytes=60 * 2**20, collective_id=0, has_side_effects=True),
        cost_estimate=pl.CostEstimate(flops=2 * rows * d_model * groups * wide, bytes_accessed=2 * d_model * quarter, transcendentals=0),
        name="tail",
    )(*parts, x, w_own, *w_mine, *w_other)


def ring(size, k):
    return [(i, (i + k) % size) for i in range(size)]


def make_step(cp_size, tp_size):
    def local_step(x, k_cache, v_cache, rope_table, norm_gain, w_qkv, b_qkv, w_out):
        groups, dim = k_cache.shape[1], k_cache.shape[2]
        rows, d_model = x.shape
        group_cols = w_qkv.shape[1] // groups
        heads = group_cols // dim
        q_heads = heads - 2
        me = lax.axis_index('cp')
        tp_me = lax.axis_index('tp')
        odd = lax.rem(me, 2)
        nat, tr = project(x, rope_table, norm_gain, w_qkv, b_qkv, heads, dim)
        nat = nat.reshape(rows, groups, heads, dim)
        tr = tr.reshape(groups, heads, dim, rows)
        k_new, v_new = nat[:, :, q_heads], nat[:, :, q_heads + 1]
        kn = k_new.transpose(1, 0, 2)
        vnt = tr[:, q_heads + 1]
        k_loc = k_cache.transpose(1, 0, 2)
        vt_loc = v_cache.transpose(1, 2, 0)

        q_own = tr[:, :q_heads]
        chips = cp_size // 2
        order = ((2, 1), (2, 0), (3, 0), (1, 0), (3, 1), (1, 1), (0, 1))

        def hop(val, j, flip):
            return lax.ppermute(val, 'cp', [(i, (i // 2 + j) % chips * 2 + (i % 2 ^ flip)) for i in range(cp_size)])

        def run(q, j, flip):
            owner = lax.rem(me // 2 + j, chips) * 2 + lax.rem(me + flip, 2)
            shifts = jnp.stack([(owner - me) * rows]).astype(jnp.int32)
            return attend([q], shifts, k_loc, vt_loc, kn, vnt, rows)[0]

        q10 = hop(q_own, -1, 0)
        q30 = hop(q_own, 1, 0)
        own = run(q_own, 0, 0)
        w_late, q10_late, own = lax.optimization_barrier((w_out, q10, own))
        q21 = hop(q10_late, -1, 1)
        q20 = hop(q21, 0, 1)
        queries = [q21, q20, q30, q10, hop(q30, 0, 1), hop(q10, 0, 1), hop(q_own, 0, 1)]

        w_rows = w_out.shape[0]
        half = w_rows // 2
        quarter = d_model // tp_size
        swap = [(i, i ^ 1) for i in range(cp_size)]
        mine, other = [], []
        for k in range(1, tp_size):
            to = lax.rem(tp_me + k, tp_size)
            piece = lax.dynamic_slice(w_late, (odd * half, to * quarter), (half, quarter))
            piece = lax.ppermute(piece, 'tp', ring(tp_size, k))
            mine.append(piece)

        parts, moving, last = [], None, own
        for n, q in enumerate(queries):
            if n == RELAYED + 2:
                q, last, moving = lax.optimization_barrier((q, last, moving))
                parts.append(hop(moving, -1, order[RELAYED][1]))
            elif n == len(order) - 1:
                q, last, mine = lax.optimization_barrier((q, last, mine))
                for piece in mine:
                    other.append(lax.ppermute(piece, 'cp', swap))
            else:
                q, last = lax.optimization_barrier((q, last))
            out = last = run(q, *order[n])
            if n == RELAYED:
                moving = hop(out, -1, 0)
            else:
                parts.append(hop(out, *order[n]))
        y = tail(parts + [own], x, w_out, mine, other, q_heads, dim)
        return y, k_new, v_new

    return local_step


def solution(mesh):
    row_spec = P(('dp', 'cp'), None)
    cache_spec = P(('dp', 'cp'), 'tp', None)
    inner = make_step(mesh.shape['cp'], mesh.shape['tp'])

    return jax.shard_map(inner, mesh=mesh, in_specs=(row_spec, cache_spec, cache_spec, row_spec, P(None), P(None, 'tp'), P('tp'), P('tp', None)), out_specs=(row_spec, cache_spec, cache_spec), check_vma=False)
```
